32 devices in a mesh: dp: 8 (over z, x), var: 4 (over y, core).
Axes of the slice: x: 2, y: 2, z: 4, core: 2. Of those that a mesh axis runs over, the one named last changes fastest.
Arguments:
- pixels: bfloat16 [8, 24, 4, 256], P('dp', 'var'), may hold values from -6 to 6
- var_ids: int32 [8, 24], P('dp', 'var'), may hold values from 0 to 90, as said below
- counts: int32 [8], P('dp'), may hold values from 3 to 24, as said below
- patch_weight: bfloat16 [91, 4, 1024], replicated, may hold values from -3 to 3
- var_embed: bfloat16 [91, 1024], replicated, may hold values from -5 to 5
- norm_gain: float32 [1024], replicated, may hold values from 0.1 to 1.9
- norm_bias: float32 [1024], replicated, may hold values from -3 to 3
- key_weight: bfloat16 [1024, 1024], P('dp'), may hold values from -0.1875 to 0.1875
- value_weight: bfloat16 [1024, 1024], P('dp'), may hold values from -0.1875 to 0.1875
- query: float32 [16, 64], replicated, may hold values from -200 to 200
- out_weight: bfloat16 [1024, 1024], replicated, may hold values from -0.1875 to 0.1875
Outputs:
- aggregated: bfloat16 [8, 256, 1024], P('dp', 'var')
The draws below stay inside these ranges and needn't reach their ends.
Inputs may be any that keep to these rules, and one draw needn't show every extreme that they name: `var_ids`: in each sample the ids of slots below its count are distinct; slots at or past the count are padding with arbitrary ids. `counts`: some sample has exactly min(91, 24) live slots and some has exactly 3.
All inputs are finite; a program needn't handle non-finite values.
Results may differ from the reference program's by a relative error of at most 0.018.
Values may be sent and summed in bfloat16 or wider, within the bound.
A program may use at most 64 MiB of HBM per device.

```python
import math
import jax
import jax.numpy as jnp
from jax import lax

D = 1024
HEADS = 16
HEAD = 64
PP = 4
VARS = 91
PW = 256
BATCH = 8
VSLOTS = 24


def draw_var_ids(key, part):
    sample_keys = jax.random.split(key, BATCH)

    def one(sample_key):
        order = jax.random.permutation(sample_key, VARS).astype(jnp.int32)
        filler = jax.random.randint(jax.random.fold_in(sample_key, 7), (VSLOTS,), 0, VARS).astype(jnp.int32)
        return jnp.concatenate([order, filler])[:VSLOTS]
    return jax.vmap(one)(sample_keys)


def draw_counts(key, part):
    highest = min(VARS, VSLOTS)
    base = jax.random.randint(jax.random.fold_in(key, 11), (BATCH,), 3, highest + 1).astype(jnp.int32)
    picked = jax.random.permutation(jax.random.fold_in(key, 13), BATCH)
    base = jnp.where(picked == 0, jnp.int32(highest), base)
    base = jnp.where(picked == 1, jnp.int32(3), base)
    return base.astype(jnp.int32)


def draw_query(key, part):
    first = jax.random.fold_in(key, 21)
    second = jax.random.fold_in(key, 23)
    base = jnp.clip(jax.random.normal(first, (HEADS, HEAD), jnp.float32), -5.0, 5.0)
    scales = jnp.exp(jax.random.uniform(second, (HEADS, 1), jnp.float32, math.log(0.5), math.log(4.0)))
    return (base * scales).astype(jnp.float32)


def block_levels(rng, extent, pieces, least, top_value):
    gain, own = 1.0, jax.random.fold_in(rng, 6)
    for position, blocks in pieces:
        heights = jnp.exp(jax.random.uniform(jax.random.fold_in(own, position), (blocks,), jnp.float32, least / len(pieces), top_value / len(pieces)))
        gain = gain * jnp.repeat(heights, extent[position] // blocks).reshape([-1 if axis == position else 1 for axis in range(len(extent))])
    return gain


def bell_draw(rng, dims, width, reach, cuts=(), kind=jnp.bfloat16):
    factor_of = block_levels(rng, dims, cuts, -0.22, 0.18) if cuts else 1.0
    values = jax.random.normal(rng, dims, jnp.float32) * width * factor_of
    return jnp.minimum(jnp.maximum(values, -reach), reach).astype(kind)


def setup_inputs(seed: int = 0) -> dict:
    splits = jax.random.split(jax.random.key(seed), 12)
    pixels = bell_draw(splits[0], (BATCH, VSLOTS, PP, PW), 1.0, 6.0, ((0, 8), (1, 4)))
    var_ids = draw_var_ids(jax.random.fold_in(splits[11], 71), 0)
    counts = draw_counts(jax.random.fold_in(splits[11], 71), 0)
    patch_weight = bell_draw(splits[3], (VARS, PP, D), PP ** -0.5, 3.0)
    var_embed = bell_draw(splits[4], (VARS, D), 1.0, 5.0)
    norm_gain = jnp.clip(1.0 + 0.18 * jax.random.normal(splits[5], (D,), jnp.float32), 0.1, 1.9)
    norm_bias = bell_draw(splits[6], (D,), 0.5, 3.0, (), jnp.float32)
    key_weight = bell_draw(splits[7], (D, D), D ** -0.5, 0.1875, ((0, 8),))
    value_weight = bell_draw(splits[8], (D, D), D ** -0.5, 0.1875, ((0, 8),))
    query = draw_query(jax.random.fold_in(splits[11], 71), 0)
    out_weight = bell_draw(splits[10], (D, D), D ** -0.5, 0.1875)
    return {"pixels": pixels, "var_ids": var_ids, "counts": counts, "patch_weight": patch_weight, "var_embed": var_embed, "norm_gain": norm_gain, "norm_bias": norm_bias, "key_weight": key_weight, "value_weight": value_weight, "query": query, "out_weight": out_weight}


def one_sample(pixels, ids, count, patch_weight, var_embed, norm_gain, norm_bias, key_weight, value_weight, query, out_weight):
    table = patch_weight[ids]
    embedded = jnp.einsum('skp,skd->spd', pixels.astype(jnp.float32), table.astype(jnp.float32))
    embedded = embedded + var_embed[ids].astype(jnp.float32)[:, None, :]
    center = embedded - lax.optimization_barrier(jnp.mean(embedded, axis=-1, keepdims=True))
    spread = lax.optimization_barrier(jnp.mean(center * center, axis=-1, keepdims=True))
    normed = (center * lax.rsqrt(spread + 1e-05) * norm_gain + norm_bias).astype(jnp.bfloat16)
    slots = normed.shape[0]
    patches = normed.shape[1]
    flat = normed.reshape(slots * patches, D)
    keys = jnp.dot(flat, key_weight, preferred_element_type=jnp.float32).reshape(slots * patches, HEADS, HEAD)
    scores = jnp.einsum('nhe,he->nh', keys, query, precision=lax.Precision.HIGHEST) * (1.0 / math.sqrt(HEAD))
    scores = scores.reshape(slots, patches, HEADS)
    live = (jnp.arange(slots, dtype=jnp.int32) < count)[:, None, None]
    scores = jnp.where(live, scores, jnp.float32(-1e+30))
    peak = lax.optimization_barrier(jnp.max(scores, axis=0))
    expo = jnp.exp(scores - peak)
    total = lax.optimization_barrier(jnp.sum(expo, axis=0))
    probs = expo.astype(jnp.bfloat16)
    values = jnp.dot(flat, value_weight, preferred_element_type=jnp.float32).astype(jnp.bfloat16)
    values = values.reshape(slots, patches, HEADS, HEAD)
    numer = jnp.einsum('sph,sphe->phe', probs.astype(jnp.float32), values.astype(jnp.float32))
    mixed = (numer / total[:, :, None]).reshape(patches, D).astype(jnp.bfloat16)
    return jnp.dot(mixed, out_weight, preferred_element_type=jnp.float32).astype(jnp.bfloat16)

def reference(pixels, var_ids, counts, patch_weight, var_embed, norm_gain, norm_bias, key_weight, value_weight, query, out_weight):

    def apply(item):
        return one_sample(item[0], item[1], item[2], patch_weight, var_embed, norm_gain, norm_bias, key_weight, value_weight, query, out_weight)
    return lax.map(apply, (pixels, var_ids, counts))
```

```python
import functools
import math

import jax
import jax.numpy as jnp
from jax import lax
from jax.experimental import pallas as pl
from jax.experimental.pallas import tpu as pltpu
from jax.sharding import PartitionSpec as P

F32 = jnp.float32
BF16 = jnp.bfloat16
EXACT = lax.Precision.HIGHEST


def rounded_up(value, unit):
    return -(-value // unit) * unit


def kernel(
    dims,
    ids_ref,
    counts_ref,
    pixels_ref,
    table_hbm,
    embed_hbm,
    gain_ref,
    bias_ref,
    key_hbm,
    value_hbm,
    query_ref,
    out_hbm,
    result_ref,
    table,
    embed,
    key_block,
    wout,
    value_all,
    fold_all,
    rows_f32,
    rows_all,
    coeff_all,
    basis,
    mix_send,
    mix_recv,
    local_sem,
    value_ss,
    value_rs,
    fold_ss,
    fold_rs,
    rows_ss,
    rows_rs,
    coeff_ss,
    coeff_rs,
    mix_ss,
    mix_rs,
):
    n, nv, groups, slots, taps, patches, width, heads, head_size = dims
    padded = rows_f32.shape[1]
    depth = key_block.shape[0]
    columns = key_block.shape[1]
    local_heads = heads // groups
    half = patches * groups // nv
    owned = patches // nv
    basis_rows = nv * (taps + 2) * padded

    b = lax.axis_index("dp")
    v = lax.axis_index("var")
    r, g = v // groups, v % groups
    pair = n % 2 == 0
    lo_size = 2 if pair else 1
    hi_size = n // lo_size
    hi, lo = b // lo_size, b % lo_size

    def remote(src, dst, ss, rs, **where):
        return pltpu.make_async_remote_copy(
            src_ref=src,
            dst_ref=dst,
            send_sem=ss,
            recv_sem=rs,
            device_id=where,
            device_id_type=pl.DeviceIdType.MESH,
        )

    barrier = pltpu.get_barrier_semaphore()
    for off in range(1, n):
        pl.semaphore_signal(
            barrier, inc=1, device_id={"dp": (b + off) % n}, device_id_type=pl.DeviceIdType.MESH
        )
    for off in range(1, nv):
        pl.semaphore_signal(
            barrier, inc=1, device_id={"var": (v + off) % nv}, device_id_type=pl.DeviceIdType.MESH
        )

    mine = pl.ds(pl.multiple_of(g * columns, columns), columns)
    get_key = pltpu.make_async_copy(key_hbm.at[:, mine], key_block, local_sem.at[0])
    get_value = pltpu.make_async_copy(value_hbm.at[:, mine], value_all.at[b], local_sem.at[1])
    get_table = pltpu.make_async_copy(table_hbm, table, local_sem.at[2])
    get_embed = pltpu.make_async_copy(embed_hbm, embed, local_sem.at[3])
    get_out = pltpu.make_async_copy(out_hbm, wout, local_sem.at[4])
    get_value.start()
    get_key.start()
    get_table.start()
    get_embed.start()
    get_out.start()

    fold_rows = fold_all.shape[1]
    pick = (
        lax.broadcasted_iota(jnp.int32, (fold_rows, heads), 1)
        == lax.broadcasted_iota(jnp.int32, (fold_rows, heads), 0) + g * local_heads
    ).astype(F32)
    own_query = jnp.dot(pick, query_ref[...], precision=EXACT, preferred_element_type=F32)
    spread_out = (
        lax.broadcasted_iota(jnp.int32, (head_size, columns), 1) % head_size
        == lax.broadcasted_iota(jnp.int32, (head_size, columns), 0)
    ).astype(F32)
    tiled = jnp.dot(own_query, spread_out, precision=EXACT, preferred_element_type=F32)
    own_head = (
        lax.broadcasted_iota(jnp.int32, (fold_rows, columns), 1) // head_size
        == lax.broadcasted_iota(jnp.int32, (fold_rows, columns), 0)
    )
    diagonal = jnp.where(own_head, tiled, 0.0) * (1.0 / math.sqrt(head_size))

    get_value.wait()
    pl.semaphore_wait(barrier, n + nv - 2)

    value_sends = []

    def send_value(owner, sem, **where):
        copy = remote(
            value_all.at[owner], value_all.at[owner], value_ss.at[sem], value_rs.at[sem], **where
        )
        copy.start()
        value_sends.append(copy)

    def value_from(owner, sem):
        return remote(
            value_all.at[owner], value_all.at[owner], value_ss.at[sem], value_rs.at[sem], dp=b
        )

    mate = hi * lo_size + (lo_size - 1 - lo)
    if pair:
        send_value(b, hi_size, dp=mate)
    for off in range(1, hi_size):
        send_value(b, off, dp=((hi + off) % hi_size) * lo_size + lo)

    get_key.wait()
    fold_all[b] = lax.dot_general(
        diagonal,
        key_block[...].astype(F32),
        (((1,), (1,)), ((), ())),
        precision=EXACT,
        preferred_element_type=F32,
    )

    rows_f32[...] = jnp.zeros_like(rows_f32)
    get_table.wait()
    get_embed.wait()
    slot_of = lax.broadcasted_iota(jnp.int32, (padded, embed.shape[0]), 0)
    wanted = jnp.full((padded, embed.shape[0]), -1, jnp.int32)
    for s in range(slots):
        rows = table[ids_ref[0, s]].astype(F32)
        for k in range(taps):
            rows_f32[k, s : s + 1, :] = rows[k : k + 1, :]
        wanted = jnp.where(slot_of == s, ids_ref[0, s], wanted)
    hot = (wanted == lax.broadcasted_iota(jnp.int32, wanted.shape, 1)).astype(BF16)
    rows_f32[taps] = jnp.dot(hot, embed[...], preferred_element_type=F32)
    rows_all[v] = rows_f32[...].astype(BF16)

    fold_sends = []
    for off in range(1, n):
        copy = remote(
            fold_all.at[b], fold_all.at[b], fold_ss.at[off], fold_rs.at[off], dp=(b + off) % n
        )
        copy.start()
        fold_sends.append(copy)

    centred = []
    for k in range(taps + 1):
        row = rows_f32[k]
        centred.append(row - jnp.mean(row, axis=-1, keepdims=True))

    rows_sends = []
    for off in range(1, nv):
        copy = remote(
            rows_all.at[v], rows_all.at[v], rows_ss.at[off], rows_rs.at[off], var=(v + off) % nv
        )
        copy.start()
        rows_sends.append(copy)

    pix = pixels_ref[0].astype(F32)
    fill = jnp.zeros((padded - slots, patches), F32)
    field = []
    for k in range(taps):
        own = [pix[s, k : k + 1, :] for s in range(slots)]
        field.append(jnp.concatenate(own + ([fill] if padded > slots else []), axis=0))
    field.append(jnp.ones((padded, patches), F32))
    variance = jnp.zeros((padded, patches), F32)
    for k in range(taps + 1):
        for m in range(k, taps + 1):
            gram = jnp.mean(centred[k] * centred[m], axis=-1, keepdims=True)
            variance += (1.0 if m == k else 2.0) * gram * (field[k] * field[m])
    scale = lax.rsqrt(jnp.maximum(variance, 0.0) + 1e-05)
    for k in range(taps + 1):
        coeff_all[v, k] = field[k] * scale

    def forward(off):
        owner = ((hi + hi_size - off) % hi_size) * lo_size + lo
        value_from(owner, off).wait_recv()
        if pair:
            send_value(owner, hi_size + off, dp=mate)

    if hi_size > 1:
        forward(1)
    coeff_sends = []
    for off in range(1, nv):
        copy = remote(
            coeff_all.at[v], coeff_all.at[v], coeff_ss.at[off], coeff_rs.at[off], var=(v + off) % nv
        )
        copy.start()
        coeff_sends.append(copy)
    for off in range(2, hi_size):
        forward(off)

    gain = gain_ref[...]
    for off in range(nv):
        src = (v + nv - off) % nv
        if off:
            remote(
                rows_all.at[src], rows_all.at[src], rows_ss.at[off], rows_rs.at[off], var=v
            ).wait_recv()
        for k in range(taps + 1):
            row = rows_all[src, k].astype(F32)
            basis[src, k] = (row - jnp.mean(row, axis=-1, keepdims=True)) * gain
        basis[src, taps + 1] = jnp.broadcast_to(bias_ref[...], (padded, width))

    for off in range(1, n):
        src = (b + n - off) % n
        remote(
            fold_all.at[src], fold_all.at[src], fold_ss.at[off], fold_rs.at[off], dp=b
        ).wait_recv()
    flat = basis[...].reshape(basis_rows, width)
    folded = jnp.concatenate([fold_all[i] for i in range(n)], axis=1)
    score_of = lax.dot_general(
        flat, folded, (((1,), (1,)), ((), ())), precision=EXACT, preferred_element_type=F32
    ).reshape(nv, taps + 2, padded, fold_rows)

    for off in range(1, nv):
        src = (v + nv - off) % nv
        remote(
            coeff_all.at[src], coeff_all.at[src], coeff_ss.at[off], coeff_rs.at[off], var=v
        ).wait_recv()
    window = pl.ds(pl.multiple_of(r * half, half), half)
    coeff = [coeff_all[:, k, :, window] for k in range(taps + 1)]
    place = lax.broadcasted_iota(jnp.int32, (nv, padded, half), 1)
    slot = lax.broadcasted_iota(jnp.int32, (nv, padded, half), 0) * slots + place
    live = (place < slots) & (slot < counts_ref[0])
    weights = []
    for h in range(local_heads):
        score = jnp.broadcast_to(score_of[:, taps + 1, :, h : h + 1], (nv, padded, half))
        for k in range(taps + 1):
            score = score + coeff[k] * score_of[:, k, :, h : h + 1]
        score = jnp.where(live, score, -1e30)
        peak = jnp.max(jnp.max(score, axis=0, keepdims=True), axis=1, keepdims=True)
        expo = jnp.exp(score - peak)
        total = jnp.sum(jnp.sum(expo, axis=0, keepdims=True), axis=1, keepdims=True)
        prob = expo / total
        parts = [prob * coeff[k] for k in range(taps + 1)] + [prob]
        weights.append(jnp.stack(parts, axis=1).reshape(basis_rows, half).astype(BF16))

    if pair:
        for off in range(hi_size):
            owner = ((hi + hi_size - off) % hi_size) * lo_size + (lo_size - 1 - lo)
            value_from(owner, hi_size + off).wait_recv()
    projected = jnp.dot(
        flat.astype(BF16),
        value_all[...].reshape(width, columns),
        preferred_element_type=F32,
    ).astype(BF16)
    mixed = jnp.concatenate(
        [
            lax.dot_general(
                weights[h],
                projected[:, h * head_size : (h + 1) * head_size],
                (((0,), (0,)), ((), ())),
                preferred_element_type=F32,
            )
            for h in range(local_heads)
        ],
        axis=1,
    ).astype(BF16)
    mix_send[...] = mixed.reshape(groups, owned, columns)

    mix_sends = []
    for off in range(1, groups):
        to = (g + off) % groups
        copy = remote(
            mix_send.at[to], mix_recv.at[g], mix_ss.at[off], mix_rs.at[off], var=r * groups + to
        )
        copy.start()
        mix_sends.append(copy)

    get_out.wait()
    total = jnp.dot(mix_send[g], wout[mine, :], preferred_element_type=F32)
    for off in range(1, groups):
        src = (g + groups - off) % groups
        remote(
            mix_send.at[src], mix_recv.at[src], mix_ss.at[off], mix_rs.at[off], var=v
        ).wait_recv()
        there = pl.ds(pl.multiple_of(src * columns, columns), columns)
        total += jnp.dot(mix_recv[src], wout[there, :], preferred_element_type=F32)
    result_ref[0] = total.astype(result_ref.dtype)

    for copy in value_sends + fold_sends + rows_sends + coeff_sends + mix_sends:
        copy.wait_send()


def on_device(
    n,
    nv,
    pixels,
    var_ids,
    counts,
    patch_weight,
    var_embed,
    norm_gain,
    norm_bias,
    key_weight,
    value_weight,
    query,
    out_weight,
):
    slots, taps, patches = pixels.shape[1:]
    width = out_weight.shape[0]
    heads, head_size = query.shape
    groups = min(nv, width // 128)
    columns = width // groups
    depth = value_weight.shape[0]
    padded = rounded_up(slots, 8)
    owned = patches // nv
    fold_rows = rounded_up(heads // groups, 8)
    vmem = pl.BlockSpec(memory_space=pltpu.VMEM)
    smem = pl.BlockSpec(memory_space=pltpu.SMEM)
    hbm = pl.BlockSpec(memory_space=pl.ANY)
    dims = (n, nv, groups, slots, taps, patches, width, heads, head_size)
    dma = pltpu.SemaphoreType.DMA
    return pl.pallas_call(
        functools.partial(kernel, dims),
        out_shape=jax.ShapeDtypeStruct((1, owned, width), BF16),
        in_specs=[smem, smem, vmem, hbm, hbm, vmem, vmem, hbm, hbm, vmem, hbm],
        out_specs=vmem,
        scratch_shapes=[
            pltpu.VMEM(patch_weight.shape, BF16),
            pltpu.VMEM(var_embed.shape, BF16),
            pltpu.VMEM((depth, columns), BF16),
            pltpu.VMEM((width, width), BF16),
            pltpu.VMEM((n, depth, columns), BF16),
            pltpu.VMEM((n, fold_rows, depth), F32),
            pltpu.VMEM((taps + 1, padded, width), F32),
            pltpu.VMEM((nv, taps + 1, padded, width), BF16),
            pltpu.VMEM((nv, taps + 1, padded, patches), F32),
            pltpu.VMEM((nv, taps + 2, padded, width), F32),
            pltpu.VMEM((groups, owned, columns), BF16),
            pltpu.VMEM((groups, owned, columns), BF16),
            dma((5,)),
            dma((n,)),
            dma((n,)),
            dma((n,)),
            dma((n,)),
            dma((nv,)),
            dma((nv,)),
            dma((nv,)),
            dma((nv,)),
            dma((groups,)),
            dma((groups,)),
        ],
        compiler_params=pltpu.CompilerParams(collective_id=0, has_side_effects=True),
    )(
        var_ids,
        counts,
        pixels,
        patch_weight,
        var_embed,
        norm_gain.reshape(1, width),
        norm_bias.reshape(1, width),
        key_weight,
        value_weight,
        query,
        out_weight,
    )


def solution(mesh):
    placed = (
        P("dp", "var", None, None),
        P("dp", "var"),
        P("dp"),
        P(),
        P(),
        P(),
        P(),
        P("dp", None),
        P("dp", None),
        P(),
        P(),
    )
    return jax.shard_map(
        functools.partial(on_device, mesh.shape["dp"], mesh.shape["var"]),
        mesh=mesh,
        in_specs=placed,
        out_specs=P("dp", "var", None),
        check_vma=False,
    )
```

```python
import functools
import math

import jax
import jax.numpy as jnp
from jax import lax
from jax.experimental import pallas as pl
from jax.experimental.pallas import tpu as pltpu
from jax.sharding import PartitionSpec as P

F32 = jnp.float32
BF16 = jnp.bfloat16
EXACT = lax.Precision.HIGHEST


def rounded_up(value, unit):
    return -(-value // unit) * unit


def kernel(
    dims,
    ids_ref,
    counts_ref,
    pixels_ref,
    table_hbm,
    embed_hbm,
    gain_ref,
    bias_ref,
    key_hbm,
    value_hbm,
    query_ref,
    out_hbm,
    result_ref,
    table,
    embed,
    key_block,
    wout,
    value_all,
    fold_all,
    rows_f32,
    ids_all,
    coeff_all,
    basis,
    mix_send,
    mix_recv,
    local_sem,
    value_ss,
    value_rs,
    fold_ss,
    fold_rs,
    ids_ss,
    ids_rs,
    coeff_ss,
    coeff_rs,
    mix_ss,
    mix_rs,
):
    n, nv, groups, slots, taps, patches, width, heads, head_size = dims
    padded = rows_f32.shape[1]
    depth = key_block.shape[0]
    parts = value_ss.shape[0] // n
    columns = key_block.shape[1]
    local_heads = heads // groups
    half = patches * groups // nv
    owned = patches // nv
    basis_rows = nv * (taps + 2) * padded

    b = lax.axis_index("dp")
    v = lax.axis_index("var")
    r, g = v // groups, v % groups
    def ahead(mask):
        return (b // 2 + mask // 2) % (n // 2) * 2 + (b % 2 + mask) % 2

    def across(mask):
        return (b // 2 + n // 2 - mask // 2) % (n // 2) * 2 + (b % 2 + mask) % 2

    def remote(src, dst, ss, rs, **where):
        return pltpu.make_async_remote_copy(
            src_ref=src,
            dst_ref=dst,
            send_sem=ss,
            recv_sem=rs,
            device_id=where,
            device_id_type=pl.DeviceIdType.MESH,
        )

    def onward(mask):
        if mask == 0:
            return [1] * (n > 1) + [m for m in range(2, n, 2)]
        return [1] * (mask % 2 == 0)

    barrier = pltpu.get_barrier_semaphore()
    for bit in onward(0):
        pl.semaphore_signal(
            barrier, inc=1, device_id={"dp": ahead(bit)}, device_id_type=pl.DeviceIdType.MESH
        )
    for off in range(1, nv):
        pl.semaphore_signal(
            barrier, inc=1, device_id={"var": (v + off) % nv}, device_id_type=pl.DeviceIdType.MESH
        )

    mine = pl.ds(pl.multiple_of(g * columns, columns), columns)
    get_key = pltpu.make_async_copy(key_hbm.at[:, mine], key_block, local_sem.at[0])
    get_value = pltpu.make_async_copy(value_hbm.at[:, mine], value_all.at[b], local_sem.at[1])
    get_table = pltpu.make_async_copy(table_hbm, table, local_sem.at[2])
    get_embed = pltpu.make_async_copy(embed_hbm, embed, local_sem.at[3])
    get_out = pltpu.make_async_copy(out_hbm, wout, local_sem.at[4])
    get_value.start()
    get_key.start()
    get_table.start()
    get_embed.start()

    fold_rows = fold_all.shape[1]
    pick = (
        lax.broadcasted_iota(jnp.int32, (fold_rows, heads), 1)
        == lax.broadcasted_iota(jnp.int32, (fold_rows, heads), 0) + g * local_heads
    ).astype(F32)
    own_query = jnp.dot(pick, query_ref[...], precision=EXACT, preferred_element_type=F32)
    spread_out = (
        lax.broadcasted_iota(jnp.int32, (head_size, columns), 1) % head_size
        == lax.broadcasted_iota(jnp.int32, (head_size, columns), 0)
    ).astype(F32)
    tiled = jnp.dot(own_query, spread_out, precision=EXACT, preferred_element_type=F32)
    own_head = (
        lax.broadcasted_iota(jnp.int32, (fold_rows, columns), 1) // head_size
        == lax.broadcasted_iota(jnp.int32, (fold_rows, columns), 0)
    )
    diagonal = jnp.where(own_head, tiled, 0.0) * (1.0 / math.sqrt(head_size))

    get_key.wait()
    fold_all[b] = lax.dot_general(
        diagonal,
        key_block[...].astype(F32),
        (((1,), (1,)), ((), ())),
        precision=EXACT,
        preferred_element_type=F32,
    )

    get_table.wait()
    get_embed.wait()
    get_out.start()
    slot_of = lax.broadcasted_iota(jnp.int32, (padded, embed.shape[0]), 0)
    entry = lax.broadcasted_iota(jnp.int32, (padded, embed.shape[0]), 1)

    def centred_rows(ids):
        wanted = jnp.full(slot_of.shape, -1, jnp.int32)
        for s in range(slots):
            rows = table[ids[s]].astype(F32)
            for k in range(taps):
                rows_f32[k, s : s + 1, :] = rows[k : k + 1, :]
            wanted = jnp.where(slot_of == s, ids[s], wanted)
        hot = (wanted == entry).astype(BF16)
        kept = [rows_f32[k] for k in range(taps)]
        kept.append(jnp.dot(hot, embed[...], preferred_element_type=F32))
        return [row - jnp.mean(row, axis=-1, keepdims=True) for row in kept]

    rows_f32[...] = jnp.zeros_like(rows_f32)

    centred = centred_rows([ids_ref[0, s] for s in range(slots)])
    pix = pixels_ref[0].astype(F32)
    fill = jnp.zeros((padded - slots, patches), F32)
    field = []
    for k in range(taps):
        own = [pix[s, k : k + 1, :] for s in range(slots)]
        field.append(jnp.concatenate(own + ([fill] if padded > slots else []), axis=0))
    field.append(jnp.ones((padded, patches), F32))
    variance = jnp.zeros((padded, patches), F32)
    for k in range(taps + 1):
        for m in range(k, taps + 1):
            gram = jnp.mean(centred[k] * centred[m], axis=-1, keepdims=True)
            variance += (1.0 if m == k else 2.0) * gram * (field[k] * field[m])
    scale = lax.rsqrt(jnp.maximum(variance, 0.0) + 1e-05)
    for k in range(taps + 1):
        coeff_all[v, k] = field[k] * scale

    get_value.wait()
    pl.semaphore_wait(barrier, len(onward(0)) + nv - 1)

    cube_sends = []

    def value_copy(mask, part, owner, to):
        piece = value_all.at[owner, pl.ds(part * (depth // parts), depth // parts)]
        sem = mask * parts + part
        return remote(piece, piece, value_ss.at[sem], value_rs.at[sem], dp=to)

    def fold_copy(mask, owner, to):
        piece = fold_all.at[owner]
        return remote(piece, piece, fold_ss.at[mask], fold_rs.at[mask], dp=to)

    def spread(make, mask):
        for bit in onward(mask):
            copy = make(mask | bit, across(mask), ahead(bit))
            copy.start()
            cube_sends.append(copy)

    def take_value(mask):
        for part in range(parts):
            value_copy(mask, part, across(mask), b).wait_recv()
            spread(lambda mask, owner, to: value_copy(mask, part, owner, to), mask)

    def take_fold(mask):
        fold_copy(mask, across(mask), b).wait_recv()
        spread(fold_copy, mask)

    relayed = sorted((m for m in range(1, n) if onward(m)), key=lambda m: (bin(m).count("1"), m))
    last = [m for m in range(1, n) if not onward(m)]

    spread(fold_copy, 0)
    for part in range(parts):
        spread(lambda mask, owner, to: value_copy(mask, part, owner, to), 0)

    ids_sends = []
    for off in range(1, nv):
        copy = remote(ids_ref, ids_all.at[v], ids_ss.at[off], ids_rs.at[off], var=(v + off) % nv)
        copy.start()
        ids_sends.append(copy)

    coeff_sends = []
    for off in range(1, nv):
        copy = remote(
            coeff_all.at[v], coeff_all.at[v], coeff_ss.at[off], coeff_rs.at[off], var=(v + off) % nv
        )
        copy.start()
        coeff_sends.append(copy)

    gain = gain_ref[...]
    for off in range(nv):
        src = (v + nv - off) % nv
        if off:
            remote(ids_ref, ids_all.at[src], ids_ss.at[off], ids_rs.at[off], var=v).wait_recv()
            centred = centred_rows([ids_all[src, 0, s] for s in range(slots)])
        for k in range(taps + 1):
            basis[src, k] = centred[k] * gain
        basis[src, taps + 1] = jnp.broadcast_to(bias_ref[...], (padded, width))

    for mask in relayed:
        take_fold(mask)
    for mask in relayed:
        take_value(mask)
    for mask in last:
        take_fold(mask)
    flat = basis[...].reshape(basis_rows, width)
    folded = jnp.concatenate([fold_all[i] for i in range(n)], axis=1)
    score_of = lax.dot_general(
        flat, folded, (((1,), (1,)), ((), ())), precision=EXACT, preferred_element_type=F32
    ).reshape(nv, taps + 2, padded, fold_rows)

    for off in range(1, nv):
        src = (v + nv - off) % nv
        remote(
            coeff_all.at[src], coeff_all.at[src], coeff_ss.at[off], coeff_rs.at[off], var=v
        ).wait_recv()
    window = pl.ds(pl.multiple_of(r * half, half), half)
    coeff = [coeff_all[:, k, :, window] for k in range(taps + 1)]
    place = lax.broadcasted_iota(jnp.int32, (nv, padded, half), 1)
    slot = lax.broadcasted_iota(jnp.int32, (nv, padded, half), 0) * slots + place
    live = (place < slots) & (slot < counts_ref[0])
    weights = []
    for h in range(local_heads):
        score = jnp.broadcast_to(score_of[:, taps + 1, :, h : h + 1], (nv, padded, half))
        for k in range(taps + 1):
            score = score + coeff[k] * score_of[:, k, :, h : h + 1]
        score = jnp.where(live, score, -1e30)
        peak = jnp.max(jnp.max(score, axis=0, keepdims=True), axis=1, keepdims=True)
        expo = jnp.exp(score - peak)
        total = jnp.sum(jnp.sum(expo, axis=0, keepdims=True), axis=1, keepdims=True)
        prob = expo / total
        terms = [prob * coeff[k] for k in range(taps + 1)] + [prob]
        weights.append(jnp.stack(terms, axis=1).reshape(basis_rows, half).astype(BF16))

    for mask in last:
        take_value(mask)
    projected = jnp.dot(
        flat.astype(BF16),
        value_all[...].reshape(width, columns),
        preferred_element_type=F32,
    ).astype(BF16)
    mixed = jnp.concatenate(
        [
            lax.dot_general(
                weights[h],
                projected[:, h * head_size : (h + 1) * head_size],
                (((0,), (0,)), ((), ())),
                preferred_element_type=F32,
            )
            for h in range(local_heads)
        ],
        axis=1,
    ).astype(BF16)
    mix_send[...] = mixed.reshape(groups, owned, columns)

    mix_sends = []
    for off in range(1, groups):
        to = (g + off) % groups
        copy = remote(
            mix_send.at[to], mix_recv.at[g], mix_ss.at[off], mix_rs.at[off], var=r * groups + to
        )
        copy.start()
        mix_sends.append(copy)

    get_out.wait()
    total = jnp.dot(mix_send[g], wout[mine, :], preferred_element_type=F32)
    for off in range(1, groups):
        src = (g + groups - off) % groups
        remote(
            mix_send.at[src], mix_recv.at[src], mix_ss.at[off], mix_rs.at[off], var=v
        ).wait_recv()
        there = pl.ds(pl.multiple_of(src * columns, columns), columns)
        total += jnp.dot(mix_recv[src], wout[there, :], preferred_element_type=F32)
    result_ref[0] = total.astype(result_ref.dtype)

    for copy in cube_sends + ids_sends + coeff_sends + mix_sends:
        copy.wait_send()


def on_device(
    n,
    nv,
    pixels,
    var_ids,
    counts,
    patch_weight,
    var_embed,
    norm_gain,
    norm_bias,
    key_weight,
    value_weight,
    query,
    out_weight,
):
    slots, taps, patches = pixels.shape[1:]
    width = out_weight.shape[0]
    heads, head_size = query.shape
    groups = min(nv, width // 128)
    columns = width // groups
    depth = value_weight.shape[0]
    padded = rounded_up(slots, 8)
    owned = patches // nv
    fold_rows = rounded_up(heads // groups, 8)
    vmem = pl.BlockSpec(memory_space=pltpu.VMEM)
    smem = pl.BlockSpec(memory_space=pltpu.SMEM)
    hbm = pl.BlockSpec(memory_space=pl.ANY)
    dims = (n, nv, groups, slots, taps, patches, width, heads, head_size)
    dma = pltpu.SemaphoreType.DMA
    parts = 1
    return pl.pallas_call(
        functools.partial(kernel, dims),
        out_shape=jax.ShapeDtypeStruct((1, owned, width), BF16),
        in_specs=[smem, smem, vmem, hbm, hbm, vmem, vmem, hbm, hbm, vmem, hbm],
        out_specs=vmem,
        scratch_shapes=[
            pltpu.VMEM(patch_weight.shape, BF16),
            pltpu.VMEM(var_embed.shape, BF16),
            pltpu.VMEM((depth, columns), BF16),
            pltpu.VMEM((width, width), BF16),
            pltpu.VMEM((n, depth, columns), BF16),
            pltpu.VMEM((n, fold_rows, depth), F32),
            pltpu.VMEM((taps, padded, width), F32),
            pltpu.SMEM((nv, 1, slots), jnp.int32),
            pltpu.VMEM((nv, taps + 1, padded, patches), F32),
            pltpu.VMEM((nv, taps + 2, padded, width), F32),
            pltpu.VMEM((groups, owned, columns), BF16),
            pltpu.VMEM((groups, owned, columns), BF16),
            dma((5,)),
            dma((n * parts,)),
            dma((n * parts,)),
            dma((n,)),
            dma((n,)),
            dma((nv,)),
            dma((nv,)),
            dma((nv,)),
            dma((nv,)),
            dma((groups,)),
            dma((groups,)),
        ],
        compiler_params=pltpu.CompilerParams(collective_id=0, has_side_effects=True),
    )(
        var_ids,
        counts,
        pixels,
        patch_weight,
        var_embed,
        norm_gain.reshape(1, width),
        norm_bias.reshape(1, width),
        key_weight,
        value_weight,
        query,
        out_weight,
    )


def solution(mesh):
    placed = (
        P("dp", "var", None, None),
        P("dp", "var"),
        P("dp"),
        P(),
        P(),
        P(),
        P(),
        P("dp", None),
        P("dp", None),
        P(),
        P(),
    )
    return jax.shard_map(
        functools.partial(on_device, mesh.shape["dp"], mesh.shape["var"]),
        mesh=mesh,
        in_specs=placed,
        out_specs=P("dp", "var", None),
        check_vma=False,
    )
```
